32 devices in a mesh: gx: 2 (over x), gy: 4 (over y, core), ha: 4 (over z).
Axes of the slice: x: 2, y: 2, z: 4, core: 2. Of those that a mesh axis runs over, the one named last changes fastest.
Arguments:
- global_state: float32 [8, 60, 16, 16], P(None, 'ha', 'gx', 'gy'), may hold values from -6 to 6
- crm_state: float32 [8, 60, 16, 1024], P(None, 'ha', 'gx', 'gy'), may hold values from -6 to 6
- mixing: float32 [8, 8], replicated, may hold values from -2 to 2
- substeps: int32 [16, 16], P('gx', 'gy'), may hold values from 1 to 8
- assignment: int32 [16, 16], P('gx', 'gy'), may hold values from 0 to 31, as said below
Outputs:
- new_global: float32 [8, 60, 16, 16], P(None, 'ha', 'gx', 'gy')
- new_crm: float32 [8, 60, 16384], P(None, None, ('gx', 'gy', 'ha'))
The draws below stay inside these ranges and needn't reach their ends.
Inputs may be any that keep to these rules, and one draw needn't show every extreme that they name: `assignment`: within each tile of 8 x 4 columns every value 0 .. 31 appears once; value // 8 is the helper index, value % 8 the slot on that helper.
All inputs are finite; a program needn't handle non-finite values.
Results may differ from the reference program's by a relative error of at most 0.0003.
Values sent between devices are 32-bit elements; how exact they have to be, the bound alone decides.
A program may use at most 64 MiB of HBM per device.

```python
import jax
import jax.numpy as jnp
from jax import lax

CX = 8
CY = 4
GF = 8
CF = 8
LEV = 60
CC = 64
MAXSUB = 8
GSUB = 4
NXG = 16
NYG = 16
SLOTS = 8
N_GX = 2
N_GY = 4


def joint_draw(key):
    base = jax.random.fold_in(key, 31)
    counts = jax.random.randint(jax.random.fold_in(base, 1), (NXG, NYG), 1, 9)
    tiles_x = NXG // CX
    tiles_y = NYG // CY
    columns = CX * CY
    helpers = columns // SLOTS
    tiled = counts.reshape(tiles_x, CX, tiles_y, CY).transpose(0, 2, 1, 3).reshape(tiles_x * tiles_y, columns)
    noise = jax.random.randint(jax.random.fold_in(base, 2), tiled.shape, 0, 64)
    score = (tiled * 64 + noise) * columns + jnp.arange(columns, dtype=jnp.int32)[None, :]
    order = jnp.argsort(-score, axis=1, stable=True)
    ranking = jnp.argsort(order, axis=1, stable=True)
    lanes = ranking % helpers
    rounds = ranking // helpers
    helper = jnp.where(rounds % 2 == 0, lanes, helpers - 1 - lanes)
    values = helper * SLOTS + rounds
    placed = values.reshape(tiles_x, tiles_y, CX, CY).transpose(0, 2, 1, 3).reshape(NXG, NYG)
    return (counts.astype(jnp.int32), placed.astype(jnp.int32))


def draw_substeps(key, part):
    return joint_draw(key)[0]


def draw_assignment(key, part):
    return joint_draw(key)[1]


def steps_of(key, dims, shards, smallest, largest):
    gain = 1.0
    for position, blocks in shards:
        steps = jax.random.uniform(jax.random.fold_in(jax.random.fold_in(key, 6), position), (blocks,), jnp.float32, smallest / len(shards), largest / len(shards))
        gain = gain * jnp.repeat(jnp.exp(steps), dims[position] // blocks).reshape((-1,) + (1,) * (len(dims) - 1 - position))
    return gain


def gaussian(own_key, extent, width, most, shards=(), held_as=jnp.bfloat16):
    drawn = jax.random.normal(own_key, extent, jnp.float32) * width
    if len(shards) > 0:
        drawn = steps_of(own_key, extent, shards, -0.22, 0.18) * drawn
    return jnp.clip(drawn, min=-most, max=most).astype(held_as)


def setup_inputs(seed: int = 0) -> dict:
    seeds = jax.random.split(jax.random.key(seed), 6)
    global_state = gaussian(seeds[0], (GF, LEV, NXG, NYG), 1.0, 6.0, ((1, 4), (2, 2), (3, 4)), jnp.float32)
    crm_state = gaussian(seeds[1], (CF, LEV, NXG, NYG * CC), 1.0, 6.0, ((1, 4), (2, 2), (3, 4)), jnp.float32)
    mixing = gaussian(seeds[2], (CF, CF), CF ** -0.5, 2.0, (), jnp.float32)
    substeps = draw_substeps(jax.random.fold_in(seeds[5], 71), 0)
    assignment = draw_assignment(jax.random.fold_in(seeds[5], 71), 0)
    return dict(global_state=global_state, crm_state=crm_state, mixing=mixing, substeps=substeps, assignment=assignment)


HIGH = lax.Precision.HIGHEST


def global_operator(field):
    east = jnp.roll(field, -1, axis=2)
    west = jnp.roll(field, 1, axis=2)
    north = jnp.roll(field, -1, axis=3)
    south = jnp.roll(field, 1, axis=3)
    return 0.2 * (east + west + north + south - 4.0 * field) - 0.15 * (east - west) - 0.15 * (north - south)


def crm_update(state, pushed, mixing):
    lateral = jnp.roll(state, 1, axis=3) + jnp.roll(state, -1, axis=3) - 2.0 * state
    upper = jnp.concatenate([state[:, :1], state[:, :-1]], axis=1)
    lower = jnp.concatenate([state[:, 1:], state[:, -1:]], axis=1)
    coupling = jnp.einsum('gf,flsc->glsc', mixing, jnp.tanh(state), precision=HIGH)
    return state + 0.1 * (1.0 * lateral + 0.5 * (upper + lower - 2.0 * state) + pushed + coupling)


def to_tiles(array, lead):
    shaped = array.reshape(array.shape[:lead] + (N_GX, CX, N_GY, CY))
    moved = jnp.moveaxis(shaped, (lead, lead + 2), (0, 1))
    return moved.reshape((N_GX * N_GY,) + array.shape[:lead] + (CX * CY,))


def from_tiles(array, lead):
    inner = array.shape[1:1 + lead]
    shaped = array.reshape((N_GX, N_GY) + inner + (CX, CY))
    moved = jnp.moveaxis(shaped, (0, 1), (lead, lead + 2))
    return moved.reshape(inner + (CX * N_GX, CY * N_GY))


def reference(global_state, crm_state, mixing, substeps, assignment):
    current = global_state
    for substep in range(GSUB):
        current = current + 0.5 * global_operator(current)
    forcing = (current - global_state) / (0.5 * GSUB)
    columns = CX * CY
    shaped = crm_state.reshape(CF, LEV, N_GX, CX, N_GY, CY, CC)
    shaped = jnp.moveaxis(shaped, (2, 4), (0, 1))
    state_tiles = shaped.reshape(N_GX * N_GY, CF, LEV, columns, CC)
    forcing_tiles = to_tiles(forcing, 2)
    count_tiles = to_tiles(substeps, 0)
    assign_tiles = to_tiles(assignment, 0)

    def per_tile(inputs):
        states, pushes, counts, assigned = inputs
        onehot = (assigned[:, None] == jnp.arange(columns, dtype=jnp.int32)[None, :]).astype(jnp.float32)
        slotted = jnp.einsum('flxc,xj->fljc', states, onehot, precision=HIGH)
        pushed = jnp.einsum('glx,xj->glj', pushes, onehot, precision=HIGH)[:, :, :, None]
        slot_counts = jnp.dot(counts.astype(jnp.float32), onehot, precision=HIGH).astype(jnp.int32)

        def one_step(index, state):
            updated = crm_update(state, pushed, mixing)
            return jnp.where((index < slot_counts)[:, None], updated, state)

        final = lax.fori_loop(0, MAXSUB, one_step, slotted)
        tendency = jnp.mean(final - slotted, axis=3)
        placed = jnp.einsum('flj,xj->flx', tendency, onehot, precision=HIGH)
        return final, placed

    finals, placed = lax.map(per_tile, (state_tiles, forcing_tiles, count_tiles, assign_tiles))
    new_crm = jnp.moveaxis(finals, 0, 2).reshape((CF, LEV, N_GX * N_GY * columns * CC))
    new_global = current + from_tiles(placed, 2)
    return new_global, new_crm
```

```python
import functools

import jax
import jax.numpy as jnp
from jax import lax
from jax.experimental import pallas as pl
from jax.experimental.pallas import tpu as pltpu
from jax.sharding import PartitionSpec as P

MAXSUB = 8
GSUB = 4
LANES = 128
CHUNK = 30
MESH = pl.DeviceIdType.MESH
HIGH = lax.Precision.HIGHEST
F32 = jnp.float32
I32 = jnp.int32


def lane_iota(shape):
    return lax.broadcasted_iota(I32, shape, len(shape) - 1)


def expand_levels(v, lane, slots, p):
    v = jnp.where(lax.div(lax.rem(lane, slots), 2) == p, v, 0.0)
    if p > 0:
        v = pltpu.roll(v, LANES - 2 * p, 1)
    shift = 2
    while shift < slots:
        v = v + pltpu.roll(v, shift, 1)
        shift *= 2
    parts = [v]
    while shift < LANES:
        clear = (lane & shift) == 0
        low = [jnp.where(clear, u, pltpu.roll(u, shift, 1)) for u in parts]
        high = [jnp.where(clear, pltpu.roll(u, LANES - shift, 1), u) for u in parts]
        parts = low + high
        shift *= 2
    return parts


def fold_levels(parts, lane, slots):
    shift = LANES // 2
    while shift >= slots:
        clear = (lane & shift) == 0
        half = len(parts) // 2
        after = []
        for a, b in zip(parts[:half], parts[half:]):
            after.append(jnp.where(
                clear, a + pltpu.roll(a, LANES - shift, 1), b + pltpu.roll(b, shift, 1)))
        parts = after
        shift //= 2
    v = parts[0]
    while shift >= 2:
        v = v + jnp.where(
            (lane & shift) == 0, pltpu.roll(v, LANES - shift, 1), pltpu.roll(v, shift, 1))
        shift //= 2
    return v


def step_kernel(
    dims, sizes, assign_ref, steps_ref, mixing_ref, g_ref, crm_ref, out_ref, newg_ref,
    raw, slots_ref, state, work, done, push, packed_g, ext, diag, g4, fcol,
    fsend, frecv, tsend, trecv, mask, table_ref,
    raw_sem, out_sem, halo_send, halo_recv, crm_send, crm_recv, f_send, f_recv, t_send, t_recv,
):
    fields, levels, tile_x, tile_y, width, helpers, pairs = dims
    n_gx, n_gy = sizes
    columns = tile_x * tile_y
    levels_all = levels * helpers
    slots = 2 * pairs
    span = LANES // tile_y
    h = GSUB
    gx, gy, ha = lax.axis_index("gx"), lax.axis_index("gy"), lax.axis_index("ha")

    offsets = [(dx, dy) for dx in (0, 1, -1) for dy in (0, 1, -1) if (dx, dy) != (0, 0)]

    def tile_at(dx, dy):
        return {"gx": lax.rem(gx + dx + n_gx, n_gx), "gy": lax.rem(gy + dy + n_gy, n_gy)}

    order = sorted(range(1, helpers), key=lambda i: -min(i, helpers - i))
    peers = [lax.rem(ha + i, helpers) for i in order]
    barrier = pltpu.get_barrier_semaphore()
    for peer in peers:
        pl.semaphore_signal(barrier, inc=1, device_id={"ha": peer}, device_id_type=MESH)
    for dx, dy in offsets:
        pl.semaphore_signal(barrier, inc=1, device_id=tile_at(dx, dy), device_id_type=MESH)
    halves = raw.shape[0]
    loads = [
        pltpu.make_async_copy(
            crm_ref.at[:, pl.ds(LANES * i, LANES)], raw.at[i], raw_sem.at[i])
        for i in range(halves)
    ]
    for copy in loads:
        copy.start()

    def find(v, carry):
        found = 0
        for x in range(tile_x):
            for y in range(tile_y):
                found = jnp.where(assign_ref[y, x] == v, x * tile_y + y, found)
        table_ref[v] = found
        table_ref[columns + v] = steps_ref[lax.rem(found, tile_y), lax.div(found, tile_y)]
        return carry

    lax.fori_loop(0, columns, find, 0)

    packed_g[...] = jnp.zeros(packed_g.shape, F32)
    for x in range(tile_x):
        for y in range(tile_y):
            packed_g[x, :, y * span:y * span + levels] = g_ref[
                pl.ds(x * tile_y + y, fields, stride=columns), :]

    lane = lane_iota((fields, LANES))
    even = lax.rem(lane, 2) == 0
    half = lax.div(lane, 2)

    def gather(q):
        ca = table_ref[2 * q]
        cb = table_ref[2 * q + 1]
        xa, ya = lax.div(ca, tile_y), lax.rem(ca, tile_y)
        xb, yb = lax.div(cb, tile_y), lax.rem(cb, tile_y)
        ia = half + lax.rem(ya, 2) * width
        ib = half + lax.rem(yb, 2) * width
        ha_, hb_ = lax.div(ya, 2), lax.div(yb, 2)
        pieces = []
        for l in range(levels):
            a = raw[ha_, pl.ds(l * tile_x + xa, fields, stride=levels * tile_x), :]
            b = raw[hb_, pl.ds(l * tile_x + xb, fields, stride=levels * tile_x), :]
            a = jnp.take_along_axis(a, ia, axis=1)
            b = jnp.take_along_axis(b, ib, axis=1)
            pieces.append(jnp.where(even, a, b))
        return pieces

    def gather_pair(p):
        for peer in peers:
            for l, piece in enumerate(gather(peer * pairs + p)):
                slots_ref[(peer * pairs + p) * levels + l] = piece

    moves = []
    for p in range(pairs):
        row = []
        for i, peer in enumerate(peers):
            row.append(pltpu.make_async_remote_copy(
                src_ref=slots_ref.at[pl.ds((peer * pairs + p) * levels, levels)],
                dst_ref=state.at[p, pl.ds(ha * levels, levels)],
                send_sem=crm_send.at[p, i], recv_sem=crm_recv.at[p, i],
                device_id={"ha": peer}, device_id_type=MESH))
        moves.append(row)

    for copy in loads:
        copy.wait()
    gather_pair(0)
    pl.semaphore_wait(barrier, len(offsets) + len(peers))
    for copy in moves[0]:
        copy.start()

    halos = []
    for o, (dx, dy) in enumerate(offsets):
        if dx == 0:
            src, dst = packed_g, ext.at[1 - dy, pl.ds(h, tile_x)]
        elif dx == 1:
            src, dst = packed_g.at[pl.ds(tile_x - h, h)], ext.at[1 - dy, pl.ds(0, h)]
        else:
            src, dst = packed_g.at[pl.ds(0, h)], ext.at[1 - dy, pl.ds(tile_x + h, h)]
        halos.append(pltpu.make_async_remote_copy(
            src_ref=src, dst_ref=dst, send_sem=halo_send.at[o], recv_sem=halo_recv.at[o],
            device_id=tile_at(dx, dy), device_id_type=MESH))
        halos[-1].start()

    for p in range(1, pairs):
        gather_pair(p)
    for p in range(pairs):
        for l, piece in enumerate(gather(ha * pairs + p)):
            state[p, ha * levels + l] = piece
    ext[1, h:h + tile_x] = packed_g[...]
    lane3 = lane_iota((1, 1, LANES))
    for copy in halos:
        copy.wait_recv()
    tiles = [ext[t] for t in range(3)]
    for _ in range(GSUB):
        up = [pltpu.roll(t, LANES - span, 2) for t in tiles]
        down = [pltpu.roll(t, span, 2) for t in tiles]
        after = []
        for t in range(3):
            north = jnp.where(lane3 < LANES - span, up[t], up[min(t + 1, 2)])
            south = jnp.where(lane3 >= span, down[t], down[max(t - 1, 0)])
            v = tiles[t]
            after.append(
                0.6 * v[1:-1] + 0.025 * (v[2:] + north[1:-1]) + 0.175 * (v[:-2] + south[1:-1]))
        tiles = after
    g4[...] = tiles[1]
    forcing = (tiles[1] - packed_g[...]) * (1.0 / (0.5 * GSUB))

    rows = lax.broadcasted_iota(I32, (LANES, LANES), 0)
    cols = lax.broadcasted_iota(I32, (LANES, LANES), 1)
    flat = forcing.reshape(tile_x * fields, LANES)
    for y in range(tile_y):
        spread = jnp.where(rows == y * span + lax.div(cols, slots), 1.0, 0.0).astype(F32)
        fcol[y] = jnp.dot(flat, spread, precision=HIGH, preferred_element_type=F32).reshape(
            tile_x, fields, LANES)
    slot_of = lax.rem(lane, slots)
    for k in range(helpers):
        packed = jnp.zeros((fields, LANES), F32)
        for j in range(slots):
            c = table_ref[k * slots + j]
            v = fcol[lax.rem(c, tile_y), lax.div(c, tile_y)]
            packed = jnp.where(slot_of == j, v, packed)
        fsend[k] = packed
    fmoves = []
    for i, peer in enumerate(peers):
        fmoves.append(pltpu.make_async_remote_copy(
            src_ref=fsend.at[peer], dst_ref=frecv.at[ha],
            send_sem=f_send.at[i], recv_sem=f_recv.at[i],
            device_id={"ha": peer}, device_id_type=MESH))
        fmoves[-1].start()
    for p in range(1, pairs):
        for copy in moves[p]:
            copy.start()
    frecv[ha] = fsend[ha]

    mix = mixing_ref[...]
    mrow = lax.broadcasted_iota(I32, (fields, fields), 0)
    mcol = lax.broadcasted_iota(I32, (fields, fields), 1)
    for k in range(fields):
        picked = jnp.where(mcol == lax.rem(mrow + k, fields), mix, 0.0)
        diag[k] = jnp.broadcast_to(
            0.1 * jnp.sum(picked, axis=1, keepdims=True), (fields, LANES))
    chunk = max(d for d in range(1, CHUNK + 1) if levels_all % d == 0)

    for copy in fmoves:
        copy.wait_recv()
    pair_of = lax.div(lax.rem(lane, slots), 2)
    for p in range(pairs):
        for z in range(helpers):
            parts = expand_levels(0.1 * frecv[z], lane, slots, p)
            for l in range(levels):
                push[p, z * levels + l] = parts[l]

    unweave = 2 * lax.rem(lane, width) + lax.div(lane, width)
    sums = [jnp.zeros((fields, LANES), F32)] * helpers
    stores = []
    for p in range(pairs):
        for copy in moves[p]:
            copy.wait_recv()
        first = ha * slots + 2 * p
        counts = jnp.where(even, table_ref[columns + first], table_ref[columns + first + 1])

        def one_step(k, source, p=p, counts=counts):
            active = k < counts

            def some_levels(b, prev):
                l0 = b * chunk
                v = [prev] + [source[p, l0 + i] for i in range(chunk)]
                v.append(source[p, jnp.minimum(l0 + chunk, levels_all - 1)])
                for i in range(chunk):
                    s = v[i + 1]
                    t = jnp.tanh(s)
                    total = diag[0] * t + push[p, l0 + i]
                    for m in range(1, fields):
                        total = total + diag[m] * pltpu.roll(t, fields - m, 0)
                    total = total + 0.1 * (pltpu.roll(s, 2, 1) + pltpu.roll(s, LANES - 2, 1))
                    total = total + 0.05 * (v[i] + v[i + 2]) + 0.7 * s
                    work[p, l0 + i] = jnp.where(active, total, s)
                return v[chunk]

            lax.fori_loop(0, levels_all // chunk, some_levels, source[p, 0])

        def later_step(k, carry):
            one_step(k, work)
            return carry

        one_step(0, state)
        lax.fori_loop(1, MAXSUB, later_step, 0)
        zero = jnp.zeros((fields, LANES), F32)
        for z in range(helpers):
            parts = [work[p, z * levels + l] - state[p, z * levels + l] for l in range(levels)]
            parts += [zero] * (LANES // slots - levels)
            sums[z] = jnp.where(pair_of == p, fold_levels(parts, lane, slots), sums[z])
        if p == pairs - 1:
            for z in range(helpers):
                tsend[z] = sums[z]
            tmoves = []
            for i, peer in enumerate(peers):
                tmoves.append(pltpu.make_async_remote_copy(
                    src_ref=tsend.at[peer], dst_ref=trecv.at[ha],
                    send_sem=t_send.at[i], recv_sem=t_recv.at[i],
                    device_id={"ha": peer}, device_id_type=MESH))
                tmoves[-1].start()
            trecv[ha] = tsend[ha]
        for l in range(levels_all):
            done[p, l] = jnp.take_along_axis(work[p, l], unweave, axis=1)
        stores.append(pltpu.make_async_copy(
            done.at[p], out_ref.at[:, :, pl.ds(p * LANES, LANES)], out_sem.at[p]))
        stores[-1].start()

    for row in moves:
        for copy in row:
            copy.wait_send()
    for copy in halos + fmoves:
        copy.wait_send()
    for copy in tmoves:
        copy.wait()
    placed = jnp.zeros((tile_x * fields, LANES), F32)
    for y in range(tile_y):
        for x in range(tile_x):
            a = assign_ref[y, x]
            v = trecv[lax.div(a, slots)]
            mask[x] = jnp.where(slot_of == lax.rem(a, slots), v, 0.0)
        pick = jnp.where(
            (cols == y * span + lax.div(rows, slots)) & (rows < levels * slots), 1.0, 0.0
        ).astype(F32)
        placed = placed + jnp.dot(
            mask[...].reshape(tile_x * fields, LANES), pick,
            precision=HIGH, preferred_element_type=F32)
    newg = g4[...] + (1.0 / width) * placed.reshape(tile_x, fields, LANES)
    for x in range(tile_x):
        for y in range(tile_y):
            newg_ref[pl.ds(x * tile_y + y, fields, stride=columns), :] = (
                newg[x][:, y * span:y * span + levels])
    for copy in stores:
        copy.wait()


def on_device(sizes, global_state, crm_state, mixing, substeps, assignment):
    n_gx, n_gy, helpers = sizes
    fields, levels = crm_state.shape[:2]
    tile_x, tile_y = assignment.shape
    width = crm_state.shape[3] // tile_y
    columns = tile_x * tile_y
    per_helper = columns // helpers
    pairs = per_helper // 2
    span = LANES // tile_y
    levels_all = levels * helpers
    assert 2 * width == LANES and tile_y == 4 and fields == 8
    assert LANES % per_helper == 0 and levels <= LANES // per_helper and levels <= span
    assert tile_x >= GSUB and tile_y >= GSUB
    dims = (fields, levels, tile_x, tile_y, width, helpers, pairs)

    g = jnp.transpose(global_state, (0, 2, 3, 1)).reshape(fields * columns, levels)
    rows = fields * levels * tile_x
    flat = crm_state.reshape(rows, tile_y * width)

    smem = pl.BlockSpec(memory_space=pltpu.SMEM)
    vmem = pl.BlockSpec(memory_space=pltpu.VMEM)
    anywhere = pl.BlockSpec(memory_space=pl.ANY)
    dma = pltpu.SemaphoreType.DMA
    vec = (fields, LANES)
    peers = helpers - 1
    new_crm, newg = pl.pallas_call(
        functools.partial(step_kernel, dims, (n_gx, n_gy)),
        out_shape=(
            jax.ShapeDtypeStruct((levels_all, fields, per_helper * width), F32),
            jax.ShapeDtypeStruct((fields * columns, levels), F32),
        ),
        in_specs=[smem, smem, vmem, vmem, anywhere],
        out_specs=(anywhere, vmem),
        scratch_shapes=[
            pltpu.VMEM((tile_y * width // LANES, rows, LANES), F32),
            pltpu.VMEM((helpers * pairs * levels,) + vec, F32),
            pltpu.VMEM((pairs, levels_all) + vec, F32),
            pltpu.VMEM((pairs, levels_all) + vec, F32),
            pltpu.VMEM((pairs, levels_all) + vec, F32),
            pltpu.VMEM((pairs, levels_all) + vec, F32),
            pltpu.VMEM((tile_x,) + vec, F32),
            pltpu.VMEM((3, tile_x + 2 * GSUB) + vec, F32),
            pltpu.VMEM((fields,) + vec, F32),
            pltpu.VMEM((tile_x,) + vec, F32),
            pltpu.VMEM((tile_y, tile_x) + vec, F32),
            pltpu.VMEM((helpers,) + vec, F32),
            pltpu.VMEM((helpers,) + vec, F32),
            pltpu.VMEM((helpers,) + vec, F32),
            pltpu.VMEM((helpers,) + vec, F32),
            pltpu.VMEM((tile_x,) + vec, F32),
            pltpu.SMEM((2 * columns,), I32),
            dma((tile_y * width // LANES,)), dma((pairs,)),
            dma((8,)), dma((8,)),
            dma((pairs, peers)), dma((pairs, peers)),
            dma((peers,)), dma((peers,)),
            dma((peers,)), dma((peers,)),
        ],
        compiler_params=pltpu.CompilerParams(collective_id=0, has_side_effects=True),
    )(assignment.T, substeps.T, mixing, g, flat)

    newg = newg.reshape(fields, tile_x, tile_y, levels)
    return jnp.transpose(newg, (0, 3, 1, 2)), jnp.transpose(new_crm, (1, 0, 2))


def solution(mesh):
    sizes = (mesh.shape["gx"], mesh.shape["gy"], mesh.shape["ha"])
    in_specs = (
        P(None, "ha", "gx", "gy"),
        P(None, "ha", "gx", "gy"),
        P(),
        P("gx", "gy"),
        P("gx", "gy"),
    )
    out_specs = (P(None, "ha", "gx", "gy"), P(None, None, ("gx", "gy", "ha")))
    return jax.shard_map(
        functools.partial(on_device, sizes),
        mesh=mesh, in_specs=in_specs, out_specs=out_specs, check_vma=False,
    )
```

```python
import functools

import jax
import jax.numpy as jnp
from jax import lax
from jax.experimental import pallas as pl
from jax.experimental.pallas import tpu as pltpu
from jax.sharding import PartitionSpec as P

MAXSUB = 8
GSUB = 4
LANES = 128
GROUP = 10
MESH = pl.DeviceIdType.MESH
HIGH = lax.Precision.HIGHEST
F32 = jnp.float32
BF16 = jnp.bfloat16
I32 = jnp.int32


def lane_iota(shape):
    return lax.broadcasted_iota(I32, shape, len(shape) - 1)


def expand_levels(v, lane, slots, p):
    v = jnp.where(lax.div(lax.rem(lane, slots), 2) == p, v, 0.0)
    if p > 0:
        v = pltpu.roll(v, LANES - 2 * p, 1)
    shift = 2
    while shift < slots:
        v = v + pltpu.roll(v, shift, 1)
        shift *= 2
    parts = [v]
    while shift < LANES:
        clear = (lane & shift) == 0
        low = [jnp.where(clear, u, pltpu.roll(u, shift, 1)) for u in parts]
        high = [jnp.where(clear, pltpu.roll(u, LANES - shift, 1), u) for u in parts]
        parts = low + high
        shift *= 2
    return parts


def fold_levels(parts, lane, slots):
    shift = LANES // 2
    while shift >= slots:
        clear = (lane & shift) == 0
        half = len(parts) // 2
        after = []
        for a, b in zip(parts[:half], parts[half:]):
            after.append(jnp.where(
                clear, a + pltpu.roll(a, LANES - shift, 1), b + pltpu.roll(b, shift, 1)))
        parts = after
        shift //= 2
    v = parts[0]
    while shift >= 2:
        v = v + jnp.where(
            (lane & shift) == 0, pltpu.roll(v, LANES - shift, 1), pltpu.roll(v, shift, 1))
        shift //= 2
    return v


def group_of(levels_all):
    return max(d for d in range(2, GROUP + 1, 2) if levels_all % d == 0)


def step_kernel(
    dims, sizes, assign_ref, steps_ref, mixing_ref, g_ref, crm_ref, out_ref, newg_ref,
    raw, slots_ref, state, one, two, push, packed_g, ext, coupling, g4, fcol,
    fsend, frecv, tsend, trecv, table_ref,
    raw_sem, halo_send, halo_recv, crm_send, crm_recv, f_send, f_recv, t_send, t_recv,
):
    fields, levels, tile_x, tile_y, width, helpers, pairs = dims
    n_gx, n_gy = sizes
    columns = tile_x * tile_y
    levels_all = levels * helpers
    group = group_of(levels_all)
    slots = 2 * pairs
    span = LANES // tile_y
    h = GSUB
    gx, gy, ha = lax.axis_index("gx"), lax.axis_index("gy"), lax.axis_index("ha")

    offsets = [(dx, dy) for dx in (0, 1, -1) for dy in (0, 1, -1) if (dx, dy) != (0, 0)]

    def tile_at(dx, dy):
        return {"gx": lax.rem(gx + dx + n_gx, n_gx), "gy": lax.rem(gy + dy + n_gy, n_gy)}

    order = sorted(range(1, helpers), key=lambda i: -min(i, helpers - i))
    peers = [lax.rem(ha + i, helpers) for i in order]
    barrier = pltpu.get_barrier_semaphore()
    for peer in peers:
        pl.semaphore_signal(barrier, inc=1, device_id={"ha": peer}, device_id_type=MESH)
    for dx, dy in offsets:
        pl.semaphore_signal(barrier, inc=1, device_id=tile_at(dx, dy), device_id_type=MESH)
    halves = raw.shape[0]
    loads = [
        pltpu.make_async_copy(
            crm_ref.at[:, pl.ds(LANES * i, LANES)], raw.at[i], raw_sem.at[i])
        for i in range(halves)
    ]
    for copy in loads:
        copy.start()

    def find(v):
        found = 0
        for x in range(tile_x):
            for y in range(tile_y):
                found = jnp.where(assign_ref[y, x] == v, x * tile_y + y, found)
        table_ref[v] = found
        table_ref[columns + v] = steps_ref[lax.rem(found, tile_y), lax.div(found, tile_y)]

    def find_first(i, carry):
        find(lax.div(i, 2) * slots + lax.rem(i, 2))
        return carry

    def find_other(i, carry):
        find(lax.div(i, slots - 2) * slots + 2 + lax.rem(i, slots - 2))
        return carry

    lax.fori_loop(0, 2 * helpers, find_first, 0)

    lane = lane_iota((fields, LANES))
    even = lax.rem(lane, 2) == 0
    half = lax.div(lane, 2)

    def gather(q):
        ca = table_ref[2 * q]
        cb = table_ref[2 * q + 1]
        xa, ya = lax.div(ca, tile_y), lax.rem(ca, tile_y)
        xb, yb = lax.div(cb, tile_y), lax.rem(cb, tile_y)
        ia = half + lax.rem(ya, 2) * width
        ib = half + lax.rem(yb, 2) * width
        ha_, hb_ = lax.div(ya, 2), lax.div(yb, 2)
        pieces = []
        for l in range(levels):
            a = raw[ha_, pl.ds(l * tile_x + xa, fields, stride=levels * tile_x), :]
            b = raw[hb_, pl.ds(l * tile_x + xb, fields, stride=levels * tile_x), :]
            a = jnp.take_along_axis(a, ia, axis=1)
            b = jnp.take_along_axis(b, ib, axis=1)
            pieces.append(jnp.where(even, a, b))
        return pieces

    def gather_pair(p):
        for peer in peers:
            for l, piece in enumerate(gather(peer * pairs + p)):
                slots_ref[(peer * pairs + p) * levels + l] = piece

    def crm_move(p, peer, lands):
        return pltpu.make_async_remote_copy(
            src_ref=slots_ref.at[pl.ds((peer * pairs + p) * levels, levels)],
            dst_ref=state.at[p, pl.ds(lands * levels, levels)],
            send_sem=crm_send.at[p, peer], recv_sem=crm_recv.at[p, lands],
            device_id={"ha": peer}, device_id_type=MESH)

    moves = [[crm_move(p, peer, ha) for peer in peers] for p in range(pairs)]
    arrivals = [[crm_move(p, peer, peer) for peer in peers] for p in range(pairs)]

    for copy in loads:
        copy.wait()
    gather_pair(0)
    pl.semaphore_wait(barrier, len(offsets) + len(peers))
    for copy in moves[0]:
        copy.start()

    packed_g[...] = jnp.zeros(packed_g.shape, F32)
    for x in range(tile_x):
        for y in range(tile_y):
            packed_g[x, :, y * span:y * span + levels] = g_ref[
                pl.ds(x * tile_y + y, fields, stride=columns), :]

    halos = []
    for o, (dx, dy) in enumerate(offsets):
        if dx == 0:
            src, dst = packed_g, ext.at[1 - dy, pl.ds(h, tile_x)]
        elif dx == 1:
            src, dst = packed_g.at[pl.ds(tile_x - h, h)], ext.at[1 - dy, pl.ds(0, h)]
        else:
            src, dst = packed_g.at[pl.ds(0, h)], ext.at[1 - dy, pl.ds(tile_x + h, h)]
        halos.append(pltpu.make_async_remote_copy(
            src_ref=src, dst_ref=dst, send_sem=halo_send.at[o], recv_sem=halo_recv.at[o],
            device_id=tile_at(dx, dy), device_id_type=MESH))
        halos[-1].start()

    lax.fori_loop(0, columns - 2 * helpers, find_other, 0)
    for p in range(1, pairs):
        gather_pair(p)
    for p in range(pairs):
        for l, piece in enumerate(gather(ha * pairs + p)):
            state[p, ha * levels + l] = piece
    ext[1, h:h + tile_x] = packed_g[...]
    lane3 = lane_iota((1, 1, LANES))
    for copy in halos:
        copy.wait_recv()
    tiles = [ext[t] for t in range(3)]
    for _ in range(GSUB):
        up = [pltpu.roll(t, LANES - span, 2) for t in tiles]
        down = [pltpu.roll(t, span, 2) for t in tiles]
        after = []
        for t in range(3):
            north = jnp.where(lane3 < LANES - span, up[t], up[min(t + 1, 2)])
            south = jnp.where(lane3 >= span, down[t], down[max(t - 1, 0)])
            v = tiles[t]
            after.append(
                0.6 * v[1:-1] + 0.025 * (v[2:] + north[1:-1]) + 0.175 * (v[:-2] + south[1:-1]))
        tiles = after
    for x in range(tile_x):
        for y in range(tile_y):
            g4[x * tile_y + y] = pltpu.roll(tiles[1][x], (LANES - y * span) % LANES, 1)
    forcing = (tiles[1] - packed_g[...]) * (1.0 / (0.5 * GSUB))

    rows = lax.broadcasted_iota(I32, (LANES, LANES), 0)
    cols = lax.broadcasted_iota(I32, (LANES, LANES), 1)
    flat = forcing.reshape(tile_x * fields, LANES)
    for y in range(tile_y):
        spread = jnp.where(rows == y * span + lax.div(cols, slots), 1.0, 0.0).astype(F32)
        fcol[y] = jnp.dot(flat, spread, precision=HIGH, preferred_element_type=F32).reshape(
            tile_x, fields, LANES)
    slot_of = lax.rem(lane, slots)
    for k in range(helpers):
        packed = jnp.zeros((fields, LANES), F32)
        for j in range(slots):
            c = table_ref[k * slots + j]
            v = fcol[lax.rem(c, tile_y), lax.div(c, tile_y)]
            packed = jnp.where(slot_of == j, v, packed)
        fsend[k] = packed
    fmoves = []
    for i, peer in enumerate(peers):
        fmoves.append(pltpu.make_async_remote_copy(
            src_ref=fsend.at[peer], dst_ref=frecv.at[ha],
            send_sem=f_send.at[i], recv_sem=f_recv.at[i],
            device_id={"ha": peer}, device_id_type=MESH))
        fmoves[-1].start()
    for p in range(1, pairs):
        for copy in moves[p]:
            copy.start()
    frecv[ha] = fsend[ha]

    mix = mixing_ref[...]
    height = group * fields
    tall = lax.broadcasted_iota(I32, (height, fields), 0)
    pick_row = jnp.where(
        lax.rem(tall, fields) == lax.broadcasted_iota(I32, (height, fields), 1), 1.0, 0.0)
    flat_row = lax.broadcasted_iota(I32, (fields, 3 * height), 0)
    flat_col = lax.broadcasted_iota(I32, (fields, 3 * height), 1)
    pick_col = jnp.where(lax.rem(flat_col, fields) == flat_row, 1.0, 0.0)
    spread_mix = jnp.dot(
        jnp.dot(pick_row.astype(F32), 0.1 * mix, precision=HIGH, preferred_element_type=F32),
        pick_col.astype(F32), precision=HIGH, preferred_element_type=F32)
    block_row = lax.broadcasted_iota(I32, (height, 3 * height), 0)
    block_col = lax.broadcasted_iota(I32, (height, 3 * height), 1)
    same = lax.div(block_row, fields) == lax.rem(lax.div(block_col, fields), group)
    spread_mix = jnp.where(same, spread_mix, 0.0)
    top = spread_mix.astype(BF16).astype(F32)
    coupling[...] = jnp.where(block_col < 2 * height, top, spread_mix - top).astype(BF16)

    for copy in fmoves:
        copy.wait_recv()
    pair_of = lax.div(lax.rem(lane, slots), 2)
    for p in range(pairs):
        for z in range(helpers):
            parts = expand_levels(0.1 * frecv[z], lane, slots, p)
            for l in range(levels):
                push[p, z * levels + l] = parts[l]

    unweave = 2 * lax.rem(lane, width) + lax.div(lane, width)
    sums = [jnp.zeros((fields, LANES), F32)] * helpers
    for p in range(pairs):
        for copy in arrivals[p]:
            copy.wait_recv()
        first = ha * slots + 2 * p
        counts = jnp.where(even, table_ref[columns + first], table_ref[columns + first + 1])

        def advance(k, read, emit, p=p, counts=counts):
            active = k < counts
            for g in range(levels_all // group):
                l0 = g * group
                t = jnp.concatenate([jnp.tanh(read(l0 + i)) for i in range(group)], axis=0)
                upper = t.astype(BF16)
                lower = (t - upper.astype(F32)).astype(BF16)
                mixed = jnp.dot(
                    coupling[...], jnp.concatenate([upper, lower, upper], axis=0),
                    preferred_element_type=F32)
                for i in range(group):
                    l = l0 + i
                    s = read(l)
                    near = read(max(l - 1, 0)) + read(min(l + 1, levels_all - 1))
                    side = pltpu.roll(s, 2, 1) + pltpu.roll(s, LANES - 2, 1)
                    total = mixed[i * fields:(i + 1) * fields] + push[p, l]
                    total = total + 0.1 * side + (0.05 * near + 0.7 * s)
                    emit(l, jnp.where(active, total, s))

        def hold(ref):
            def store(l, v):
                ref[l] = v
            return store

        def two_steps(i, carry):
            advance(2 * i + 1, lambda l: one[l], hold(two))
            advance(2 * i + 2, lambda l: two[l], hold(one))
            return carry

        grown = []

        def finish(l, v, p=p):
            two[l] = v
            grown.append(v - state[p, l])

        advance(0, lambda l: state[p, l], hold(one))
        if p < pairs - 1:
            lax.fori_loop(0, MAXSUB // 2 - 1, two_steps, 0)
        else:
            for i in range(MAXSUB // 2 - 1):
                two_steps(i, 0)
        advance(MAXSUB - 1, lambda l: one[l], finish)
        zero = jnp.zeros((fields, LANES), F32)
        for z in range(helpers):
            parts = grown[z * levels:(z + 1) * levels] + [zero] * (LANES // slots - levels)
            sums[z] = jnp.where(pair_of == p, fold_levels(parts, lane, slots), sums[z])
        if p == pairs - 1:
            for z in range(helpers):
                tsend[z] = sums[z]
            tmoves = []
            for i, peer in enumerate(peers):
                tmoves.append(pltpu.make_async_remote_copy(
                    src_ref=tsend.at[peer], dst_ref=trecv.at[ha],
                    send_sem=t_send.at[i], recv_sem=t_recv.at[i],
                    device_id={"ha": peer}, device_id_type=MESH))
                tmoves[-1].start()
            trecv[ha] = tsend[ha]
        for l in range(levels_all):
            out_ref[l, :, p * LANES:(p + 1) * LANES] = jnp.take_along_axis(
                two[l], unweave, axis=1)

    for row in moves:
        for copy in row:
            copy.wait_send()
    for copy in halos + fmoves:
        copy.wait_send()
    for copy in tmoves:
        copy.wait()
    for x in range(tile_x):
        for y in range(tile_y):
            c = x * tile_y + y
            a = assign_ref[y, x]
            where = jnp.minimum(lane * slots + lax.rem(a, slots), LANES - 1)
            mean = (1.0 / width) * jnp.take_along_axis(trecv[lax.div(a, slots)], where, axis=1)
            newg_ref[pl.ds(c, fields, stride=columns), :] = (g4[c] + mean)[:, :levels]


def write_kernel(pieces, crm_ref, newg_ref, crm_out, newg_out, sem):
    step = crm_ref.shape[0] // pieces
    copies = [pltpu.make_async_copy(newg_ref, newg_out, sem.at[pieces])]
    for i in range(pieces):
        rows = pl.ds(i * step, step)
        copies.append(pltpu.make_async_copy(crm_ref.at[rows], crm_out.at[rows], sem.at[i]))
    for copy in copies:
        copy.start()
    for copy in copies:
        copy.wait()


def on_device(sizes, global_state, crm_state, mixing, substeps, assignment):
    n_gx, n_gy, helpers = sizes
    fields, levels = crm_state.shape[:2]
    tile_x, tile_y = assignment.shape
    width = crm_state.shape[3] // tile_y
    columns = tile_x * tile_y
    per_helper = columns // helpers
    pairs = per_helper // 2
    span = LANES // tile_y
    levels_all = levels * helpers
    assert 2 * width == LANES and tile_y == 4 and fields == 8
    assert LANES % per_helper == 0 and levels <= LANES // per_helper and levels <= span
    assert tile_x >= GSUB and tile_y >= GSUB
    assert levels_all % 2 == 0 and MAXSUB % 2 == 0
    dims = (fields, levels, tile_x, tile_y, width, helpers, pairs)
    group = group_of(levels_all)

    g = jnp.transpose(global_state, (0, 2, 3, 1)).reshape(fields * columns, levels)
    rows = fields * levels * tile_x
    flat = crm_state.reshape(rows, tile_y * width)

    smem = pl.BlockSpec(memory_space=pltpu.SMEM)
    vmem = pl.BlockSpec(memory_space=pltpu.VMEM)
    anywhere = pl.BlockSpec(memory_space=pl.ANY)
    dma = pltpu.SemaphoreType.DMA
    vec = (fields, LANES)
    peers = helpers - 1
    new_crm, newg = pl.pallas_call(
        functools.partial(step_kernel, dims, (n_gx, n_gy)),
        out_shape=(
            pltpu.VMEM((levels_all, fields, per_helper * width), F32),
            pltpu.VMEM((fields * columns, levels), F32),
        ),
        in_specs=[smem, smem, vmem, vmem, anywhere],
        out_specs=(vmem, vmem),
        scratch_shapes=[
            pltpu.VMEM((tile_y * width // LANES, rows, LANES), F32),
            pltpu.VMEM((helpers * pairs * levels,) + vec, F32),
            pltpu.VMEM((pairs, levels_all) + vec, F32),
            pltpu.VMEM((levels_all,) + vec, F32),
            pltpu.VMEM((levels_all,) + vec, F32),
            pltpu.VMEM((pairs, levels_all) + vec, F32),
            pltpu.VMEM((tile_x,) + vec, F32),
            pltpu.VMEM((3, tile_x + 2 * GSUB) + vec, F32),
            pltpu.VMEM((group * fields, 3 * group * fields), BF16),
            pltpu.VMEM((columns,) + vec, F32),
            pltpu.VMEM((tile_y, tile_x) + vec, F32),
            pltpu.VMEM((helpers,) + vec, F32),
            pltpu.VMEM((helpers,) + vec, F32),
            pltpu.VMEM((helpers,) + vec, F32),
            pltpu.VMEM((helpers,) + vec, F32),
            pltpu.SMEM((2 * columns,), I32),
            dma((tile_y * width // LANES,)),
            dma((8,)), dma((8,)),
            dma((pairs, helpers)), dma((pairs, helpers)),
            dma((peers,)), dma((peers,)),
            dma((peers,)), dma((peers,)),
        ],
        compiler_params=pltpu.CompilerParams(collective_id=0, has_side_effects=True),
    )(assignment.T, substeps.T, mixing, g, flat)

    pieces = 4 if levels_all % 4 == 0 else 1
    new_crm, newg = pl.pallas_call(
        functools.partial(write_kernel, pieces),
        out_shape=(
            jax.ShapeDtypeStruct((levels_all, fields, per_helper * width), F32),
            jax.ShapeDtypeStruct((fields * columns, levels), F32),
        ),
        in_specs=[anywhere, anywhere],
        out_specs=(anywhere, anywhere),
        scratch_shapes=[dma((pieces + 1,))],
    )(pltpu.with_memory_space_constraint(new_crm, pltpu.VMEM), pltpu.with_memory_space_constraint(newg, pltpu.VMEM))

    newg = newg.reshape(fields, tile_x, tile_y, levels)
    return jnp.transpose(newg, (0, 3, 1, 2)), jnp.transpose(new_crm, (1, 0, 2))


def solution(mesh):
    sizes = (mesh.shape["gx"], mesh.shape["gy"], mesh.shape["ha"])
    in_specs = (
        P(None, "ha", "gx", "gy"),
        P(None, "ha", "gx", "gy"),
        P(),
        P("gx", "gy"),
        P("gx", "gy"),
    )
    out_specs = (P(None, "ha", "gx", "gy"), P(None, None, ("gx", "gy", "ha")))
    return jax.shard_map(
        functools.partial(on_device, sizes),
        mesh=mesh, in_specs=in_specs, out_specs=out_specs, check_vma=False,
    )
```

```python
import functools

import jax
import jax.numpy as jnp
from jax import lax
from jax.experimental import pallas as pl
from jax.experimental.pallas import tpu as pltpu
from jax.sharding import PartitionSpec as P

MAXSUB = 8
GSUB = 4
LANES = 128
GROUP = 2
MESH = pl.DeviceIdType.MESH
HIGH = lax.Precision.HIGHEST
F32 = jnp.float32
BF16 = jnp.bfloat16
I32 = jnp.int32


def lane_iota(shape):
    return lax.broadcasted_iota(I32, shape, len(shape) - 1)


def expand_levels(v, lane, slots, p):
    v = jnp.where(lax.div(lax.rem(lane, slots), 2) == p, v, 0.0)
    if p > 0:
        v = pltpu.roll(v, LANES - 2 * p, 1)
    shift = 2
    while shift < slots:
        v = v + pltpu.roll(v, shift, 1)
        shift *= 2
    parts = [v]
    while shift < LANES:
        clear = (lane & shift) == 0
        low = [jnp.where(clear, u, pltpu.roll(u, shift, 1)) for u in parts]
        high = [jnp.where(clear, pltpu.roll(u, LANES - shift, 1), u) for u in parts]
        parts = low + high
        shift *= 2
    return parts


def fold_levels(parts, lane, slots):
    shift = LANES // 2
    while shift >= slots:
        clear = (lane & shift) == 0
        half = len(parts) // 2
        after = []
        for a, b in zip(parts[:half], parts[half:]):
            after.append(jnp.where(
                clear, a + pltpu.roll(a, LANES - shift, 1), b + pltpu.roll(b, shift, 1)))
        parts = after
        shift //= 2
    v = parts[0]
    while shift >= 2:
        v = v + jnp.where(
            (lane & shift) == 0, pltpu.roll(v, LANES - shift, 1), pltpu.roll(v, shift, 1))
        shift //= 2
    return v


def group_of(levels_all):
    return max(d for d in range(2, GROUP + 1, 2) if levels_all % d == 0)


def step_kernel(
    dims, sizes, assign_ref, steps_ref, mixing_ref, g_ref, crm_ref, out_ref, newg_ref,
    raw, slots_ref, state, one, two, push, packed_g, ext, coupling, g4, fcol,
    fsend, frecv, tsend, trecv, table_ref,
    raw_sem, halo_send, halo_recv, crm_send, crm_recv, f_send, f_recv, t_send, t_recv,
):
    fields, levels, tile_x, tile_y, width, helpers, pairs = dims
    n_gx, n_gy = sizes
    columns = tile_x * tile_y
    levels_all = levels * helpers
    group = group_of(levels_all)
    slots = 2 * pairs
    span = LANES // tile_y
    h = GSUB
    gx, gy, ha = lax.axis_index("gx"), lax.axis_index("gy"), lax.axis_index("ha")

    offsets = [(dx, dy) for dx in (0, 1, -1) for dy in (0, 1, -1) if (dx, dy) != (0, 0)]

    def tile_at(dx, dy):
        return {"gx": lax.rem(gx + dx + n_gx, n_gx), "gy": lax.rem(gy + dy + n_gy, n_gy)}

    order = sorted(range(1, helpers), key=lambda i: -min(i, helpers - i))
    peers = [lax.rem(ha + i, helpers) for i in order]
    barrier = pltpu.get_barrier_semaphore()
    for peer in peers:
        pl.semaphore_signal(barrier, inc=1, device_id={"ha": peer}, device_id_type=MESH)
    for dx, dy in offsets:
        pl.semaphore_signal(barrier, inc=1, device_id=tile_at(dx, dy), device_id_type=MESH)
    halves = raw.shape[0]
    loads = [
        pltpu.make_async_copy(
            crm_ref.at[:, pl.ds(LANES * i, LANES)], raw.at[i], raw_sem.at[i])
        for i in range(halves)
    ]
    for copy in loads:
        copy.start()

    def find(v):
        found = 0
        for x in range(tile_x):
            for y in range(tile_y):
                found = jnp.where(assign_ref[y, x] == v, x * tile_y + y, found)
        table_ref[v] = found
        table_ref[columns + v] = steps_ref[lax.rem(found, tile_y), lax.div(found, tile_y)]

    def find_first(i, carry):
        find(lax.div(i, 2) * slots + lax.rem(i, 2))
        return carry

    def find_other(i, carry):
        find(lax.div(i, slots - 2) * slots + 2 + lax.rem(i, slots - 2))
        return carry

    lax.fori_loop(0, 2 * helpers, find_first, 0)

    lane = lane_iota((fields, LANES))
    even = lax.rem(lane, 2) == 0
    half = lax.div(lane, 2)

    def gather(q):
        ca = table_ref[2 * q]
        cb = table_ref[2 * q + 1]
        xa, ya = lax.div(ca, tile_y), lax.rem(ca, tile_y)
        xb, yb = lax.div(cb, tile_y), lax.rem(cb, tile_y)
        ia = half + lax.rem(ya, 2) * width
        ib = half + lax.rem(yb, 2) * width
        ha_, hb_ = lax.div(ya, 2), lax.div(yb, 2)
        pieces = []
        for l in range(levels):
            a = raw[ha_, pl.ds(l * tile_x + xa, fields, stride=levels * tile_x), :]
            b = raw[hb_, pl.ds(l * tile_x + xb, fields, stride=levels * tile_x), :]
            a = jnp.take_along_axis(a, ia, axis=1)
            b = jnp.take_along_axis(b, ib, axis=1)
            pieces.append(jnp.where(even, a, b))
        return pieces

    def gather_pair(p):
        for peer in peers:
            for l, piece in enumerate(gather(peer * pairs + p)):
                slots_ref[(peer * pairs + p) * levels + l] = piece

    def crm_move(p, peer, lands):
        return pltpu.make_async_remote_copy(
            src_ref=slots_ref.at[pl.ds((peer * pairs + p) * levels, levels)],
            dst_ref=state.at[p, pl.ds(lands * levels, levels)],
            send_sem=crm_send.at[p, peer], recv_sem=crm_recv.at[p, lands],
            device_id={"ha": peer}, device_id_type=MESH)

    def send_pair(p):
        for reach in range(helpers - 1, 0, -1):
            for shift in (reach, -reach):
                @pl.when((ha + shift >= 0) & (ha + shift < helpers))
                def _():
                    crm_move(p, lax.rem(ha + shift + helpers, helpers), ha).start()

    moves = [[crm_move(p, peer, ha) for peer in peers] for p in range(pairs)]
    arrivals = [[crm_move(p, peer, peer) for peer in peers] for p in range(pairs)]

    for copy in loads:
        copy.wait()
    gather_pair(0)
    pl.semaphore_wait(barrier, len(offsets) + len(peers))
    send_pair(0)

    packed_g[...] = jnp.zeros(packed_g.shape, F32)
    for x in range(tile_x):
        for y in range(tile_y):
            packed_g[x, :, y * span:y * span + levels] = g_ref[
                pl.ds(x * tile_y + y, fields, stride=columns), :]

    halos = []
    for o, (dx, dy) in enumerate(offsets):
        if dx == 0:
            src, dst = packed_g, ext.at[1 - dy, pl.ds(h, tile_x)]
        elif dx == 1:
            src, dst = packed_g.at[pl.ds(tile_x - h, h)], ext.at[1 - dy, pl.ds(0, h)]
        else:
            src, dst = packed_g.at[pl.ds(0, h)], ext.at[1 - dy, pl.ds(tile_x + h, h)]
        halos.append(pltpu.make_async_remote_copy(
            src_ref=src, dst_ref=dst, send_sem=halo_send.at[o], recv_sem=halo_recv.at[o],
            device_id=tile_at(dx, dy), device_id_type=MESH))
        halos[-1].start()

    lax.fori_loop(0, columns - 2 * helpers, find_other, 0)
    for p in range(1, pairs):
        gather_pair(p)
    for p in range(pairs):
        for l, piece in enumerate(gather(ha * pairs + p)):
            state[p, ha * levels + l] = piece
    ext[1, h:h + tile_x] = packed_g[...]
    lane3 = lane_iota((1, 1, LANES))
    for copy in halos:
        copy.wait_recv()
    tiles = [ext[t] for t in range(3)]
    for _ in range(GSUB):
        up = [pltpu.roll(t, LANES - span, 2) for t in tiles]
        down = [pltpu.roll(t, span, 2) for t in tiles]
        after = []
        for t in range(3):
            north = jnp.where(lane3 < LANES - span, up[t], up[min(t + 1, 2)])
            south = jnp.where(lane3 >= span, down[t], down[max(t - 1, 0)])
            v = tiles[t]
            after.append(
                0.6 * v[1:-1] + 0.025 * (v[2:] + north[1:-1]) + 0.175 * (v[:-2] + south[1:-1]))
        tiles = after
    for x in range(tile_x):
        for y in range(tile_y):
            g4[x * tile_y + y] = pltpu.roll(tiles[1][x], (LANES - y * span) % LANES, 1)
    forcing = (tiles[1] - packed_g[...]) * (1.0 / (0.5 * GSUB))

    rows = lax.broadcasted_iota(I32, (LANES, LANES), 0)
    cols = lax.broadcasted_iota(I32, (LANES, LANES), 1)
    flat = forcing.reshape(tile_x * fields, LANES)
    for y in range(tile_y):
        spread = jnp.where(rows == y * span + lax.div(cols, slots), 1.0, 0.0).astype(F32)
        fcol[y] = jnp.dot(flat, spread, precision=HIGH, preferred_element_type=F32).reshape(
            tile_x, fields, LANES)
    slot_of = lax.rem(lane, slots)
    for k in range(helpers):
        packed = jnp.zeros((fields, LANES), F32)
        for j in range(slots):
            c = table_ref[k * slots + j]
            v = fcol[lax.rem(c, tile_y), lax.div(c, tile_y)]
            packed = jnp.where(slot_of == j, v, packed)
        fsend[k] = packed
    fmoves = []
    for i, peer in enumerate(peers):
        fmoves.append(pltpu.make_async_remote_copy(
            src_ref=fsend.at[peer], dst_ref=frecv.at[ha],
            send_sem=f_send.at[i], recv_sem=f_recv.at[i],
            device_id={"ha": peer}, device_id_type=MESH))
        fmoves[-1].start()
    for p in range(1, pairs):
        send_pair(p)
    frecv[ha] = fsend[ha]

    mix = mixing_ref[...]
    height = group * fields
    tall = lax.broadcasted_iota(I32, (height, fields), 0)
    pick_row = jnp.where(
        lax.rem(tall, fields) == lax.broadcasted_iota(I32, (height, fields), 1), 1.0, 0.0)
    flat_row = lax.broadcasted_iota(I32, (fields, 3 * height), 0)
    flat_col = lax.broadcasted_iota(I32, (fields, 3 * height), 1)
    pick_col = jnp.where(lax.rem(flat_col, fields) == flat_row, 1.0, 0.0)
    spread_mix = jnp.dot(
        jnp.dot(pick_row.astype(F32), 0.1 * mix, precision=HIGH, preferred_element_type=F32),
        pick_col.astype(F32), precision=HIGH, preferred_element_type=F32)
    block_row = lax.broadcasted_iota(I32, (height, 3 * height), 0)
    block_col = lax.broadcasted_iota(I32, (height, 3 * height), 1)
    same = lax.div(block_row, fields) == lax.rem(lax.div(block_col, fields), group)
    spread_mix = jnp.where(same, spread_mix, 0.0)
    top = spread_mix.astype(BF16).astype(F32)
    coupling[...] = jnp.where(block_col < 2 * height, top, spread_mix - top).astype(BF16)

    for copy in fmoves:
        copy.wait_recv()
    pair_of = lax.div(lax.rem(lane, slots), 2)
    for p in range(pairs):
        for z in range(helpers):
            parts = expand_levels(0.1 * frecv[z], lane, slots, p)
            for l in range(levels):
                push[p, z * levels + l] = parts[l]

    unweave = 2 * lax.rem(lane, width) + lax.div(lane, width)
    sums = [jnp.zeros((fields, LANES), F32)] * helpers
    for p in range(pairs):
        for copy in arrivals[p]:
            copy.wait_recv()
        first = ha * slots + 2 * p
        counts = jnp.where(even, table_ref[columns + first], table_ref[columns + first + 1])

        def advance(k, read, emit, p=p, counts=counts):
            active = k < counts
            for g in range(levels_all // group):
                l0 = g * group
                t = jnp.concatenate([jnp.tanh(read(l0 + i)) for i in range(group)], axis=0)
                upper = t.astype(BF16)
                lower = (t - upper.astype(F32)).astype(BF16)
                mixed = jnp.dot(
                    coupling[...], jnp.concatenate([upper, lower, upper], axis=0),
                    preferred_element_type=F32)
                for i in range(group):
                    l = l0 + i
                    s = read(l)
                    near = read(max(l - 1, 0)) + read(min(l + 1, levels_all - 1))
                    side = pltpu.roll(s, 2, 1) + pltpu.roll(s, LANES - 2, 1)
                    total = mixed[i * fields:(i + 1) * fields] + push[p, l]
                    total = total + 0.1 * side + (0.05 * near + 0.7 * s)
                    emit(l, jnp.where(active, total, s))

        def hold(ref):
            def store(l, v):
                ref[l] = v
            return store

        def two_steps(i, carry):
            advance(2 * i + 1, lambda l: one[l], hold(two))
            advance(2 * i + 2, lambda l: two[l], hold(one))
            return carry

        grown = []

        def finish(l, v, p=p):
            two[l] = v
            grown.append(v - state[p, l])

        advance(0, lambda l: state[p, l], hold(one))
        if p < pairs - 1:
            lax.fori_loop(0, MAXSUB // 2 - 1, two_steps, 0)
        else:
            for i in range(MAXSUB // 2 - 1):
                two_steps(i, 0)
        advance(MAXSUB - 1, lambda l: one[l], finish)
        zero = jnp.zeros((fields, LANES), F32)
        for z in range(helpers):
            parts = grown[z * levels:(z + 1) * levels] + [zero] * (LANES // slots - levels)
            sums[z] = jnp.where(pair_of == p, fold_levels(parts, lane, slots), sums[z])
        if p == pairs - 1:
            for z in range(helpers):
                tsend[z] = sums[z]
            tmoves = []
            for i, peer in enumerate(peers):
                tmoves.append(pltpu.make_async_remote_copy(
                    src_ref=tsend.at[peer], dst_ref=trecv.at[ha],
                    send_sem=t_send.at[i], recv_sem=t_recv.at[i],
                    device_id={"ha": peer}, device_id_type=MESH))
                tmoves[-1].start()
            trecv[ha] = tsend[ha]
        for l in range(levels_all):
            out_ref[l, :, p * LANES:(p + 1) * LANES] = jnp.take_along_axis(
                two[l], unweave, axis=1)

    for row in moves:
        for copy in row:
            copy.wait_send()
    for copy in halos + fmoves:
        copy.wait_send()
    for copy in tmoves:
        copy.wait()
    for x in range(tile_x):
        for y in range(tile_y):
            c = x * tile_y + y
            a = assign_ref[y, x]
            where = jnp.minimum(lane * slots + lax.rem(a, slots), LANES - 1)
            mean = (1.0 / width) * jnp.take_along_axis(trecv[lax.div(a, slots)], where, axis=1)
            newg_ref[pl.ds(c, fields, stride=columns), :] = (g4[c] + mean)[:, :levels]


def write_kernel(pieces, crm_ref, newg_ref, crm_out, newg_out, sem):
    step = crm_ref.shape[0] // pieces
    copies = [pltpu.make_async_copy(newg_ref, newg_out, sem.at[pieces])]
    for i in range(pieces):
        rows = pl.ds(i * step, step)
        copies.append(pltpu.make_async_copy(crm_ref.at[rows], crm_out.at[rows], sem.at[i]))
    for copy in copies:
        copy.start()
    for copy in copies:
        copy.wait()


def on_device(sizes, global_state, crm_state, mixing, substeps, assignment):
    n_gx, n_gy, helpers = sizes
    fields, levels = crm_state.shape[:2]
    tile_x, tile_y = assignment.shape
    width = crm_state.shape[3] // tile_y
    columns = tile_x * tile_y
    per_helper = columns // helpers
    pairs = per_helper // 2
    span = LANES // tile_y
    levels_all = levels * helpers
    assert 2 * width == LANES and tile_y == 4 and fields == 8
    assert LANES % per_helper == 0 and levels <= LANES // per_helper and levels <= span
    assert tile_x >= GSUB and tile_y >= GSUB
    assert levels_all % 2 == 0 and MAXSUB % 2 == 0
    dims = (fields, levels, tile_x, tile_y, width, helpers, pairs)
    group = group_of(levels_all)

    g = jnp.transpose(global_state, (0, 2, 3, 1)).reshape(fields * columns, levels)
    rows = fields * levels * tile_x
    flat = crm_state.reshape(rows, tile_y * width)

    smem = pl.BlockSpec(memory_space=pltpu.SMEM)
    vmem = pl.BlockSpec(memory_space=pltpu.VMEM)
    anywhere = pl.BlockSpec(memory_space=pl.ANY)
    dma = pltpu.SemaphoreType.DMA
    vec = (fields, LANES)
    peers = helpers - 1
    new_crm, newg = pl.pallas_call(
        functools.partial(step_kernel, dims, (n_gx, n_gy)),
        out_shape=(
            pltpu.VMEM((levels_all, fields, per_helper * width), F32),
            pltpu.VMEM((fields * columns, levels), F32),
        ),
        in_specs=[smem, smem, vmem, vmem, anywhere],
        out_specs=(vmem, vmem),
        scratch_shapes=[
            pltpu.VMEM((tile_y * width // LANES, rows, LANES), F32),
            pltpu.VMEM((helpers * pairs * levels,) + vec, F32),
            pltpu.VMEM((pairs, levels_all) + vec, F32),
            pltpu.VMEM((levels_all,) + vec, F32),
            pltpu.VMEM((levels_all,) + vec, F32),
            pltpu.VMEM((pairs, levels_all) + vec, F32),
            pltpu.VMEM((tile_x,) + vec, F32),
            pltpu.VMEM((3, tile_x + 2 * GSUB) + vec, F32),
            pltpu.VMEM((group * fields, 3 * group * fields), BF16),
            pltpu.VMEM((columns,) + vec, F32),
            pltpu.VMEM((tile_y, tile_x) + vec, F32),
            pltpu.VMEM((helpers,) + vec, F32),
            pltpu.VMEM((helpers,) + vec, F32),
            pltpu.VMEM((helpers,) + vec, F32),
            pltpu.VMEM((helpers,) + vec, F32),
            pltpu.SMEM((2 * columns,), I32),
            dma((tile_y * width // LANES,)),
            dma((8,)), dma((8,)),
            dma((pairs, helpers)), dma((pairs, helpers)),
            dma((peers,)), dma((peers,)),
            dma((peers,)), dma((peers,)),
        ],
        compiler_params=pltpu.CompilerParams(collective_id=0, has_side_effects=True),
    )(assignment.T, substeps.T, mixing, g, flat)

    pieces = 4 if levels_all % 4 == 0 else 1
    new_crm, newg = pl.pallas_call(
        functools.partial(write_kernel, pieces),
        out_shape=(
            jax.ShapeDtypeStruct((levels_all, fields, per_helper * width), F32),
            jax.ShapeDtypeStruct((fields * columns, levels), F32),
        ),
        in_specs=[anywhere, anywhere],
        out_specs=(anywhere, anywhere),
        scratch_shapes=[dma((pieces + 1,))],
    )(pltpu.with_memory_space_constraint(new_crm, pltpu.VMEM), pltpu.with_memory_space_constraint(newg, pltpu.VMEM))

    newg = newg.reshape(fields, tile_x, tile_y, levels)
    return jnp.transpose(newg, (0, 3, 1, 2)), jnp.transpose(new_crm, (1, 0, 2))


def solution(mesh):
    sizes = (mesh.shape["gx"], mesh.shape["gy"], mesh.shape["ha"])
    in_specs = (
        P(None, "ha", "gx", "gy"),
        P(None, "ha", "gx", "gy"),
        P(),
        P("gx", "gy"),
        P("gx", "gy"),
    )
    out_specs = (P(None, "ha", "gx", "gy"), P(None, None, ("gx", "gy", "ha")))
    return jax.shard_map(
        functools.partial(on_device, sizes),
        mesh=mesh, in_specs=in_specs, out_specs=out_specs, check_vma=False,
    )
```
